32 devices in a mesh: gx: 16 (over z, x, core), gy: 2 (over y).
Axes of the slice: x: 2, y: 2, z: 4, core: 2. Of those that a mesh axis runs over, the one named last changes fastest.
Arguments:
- volt: float32 [128, 128, 2048], P('gx', 'gy'), may hold values from -6 to 6
- drive: float32 [128, 128, 2048], P('gx', 'gy'), may hold values from -6 to 6
- region: int32 [128, 128, 32], P('gx', 'gy'), may hold values from 0 to 7
- diode_mask: int32 [128, 128, 32], P('gx', 'gy'), may hold values 0 or 1
- sigma_table: float32 [8], replicated, may hold values from 0.3 to 3
- cap_table: float32 [8], replicated, may hold values from 0.1 to 1
Outputs:
- residual: float32 [128, 128, 2048], P('gx', 'gy')
- coef_norms: float32 [64], replicated
The draws below stay inside these ranges and needn't reach their ends.
All inputs are finite; a program needn't handle non-finite values. No bound on the sum of `diode_mask` on one device may be relied on, other than what follows from the above.
Results may differ from the reference program's by a relative error of at most 0.0003.
Values sent between devices are 32-bit elements; how exact they have to be, the bound alone decides.
A program may use at most 192 MiB of HBM per device.

```python
import math
import jax
import jax.numpy as jnp
from jax import lax

NZ = 32
H = 32
KC = 64
S = 256
REGIONS = 8
NX = 128
NY = 128


def with_ends(values, key, least, high):
    extent = values.shape
    place = [jax.random.randint(jax.random.fold_in(key, axis), (), 0, extent[axis]) for axis in range(len(extent))]
    values = values.at[tuple(place)].set(least)
    longest = extent.index(max(extent))
    place[longest] = (place[longest] + 1) % extent[longest]
    return values.at[tuple(place)].set(high)


def shard_levels(rng, shape, shards, least, high):
    def one(dim, shards_of):
        draws = jax.random.uniform(jax.random.fold_in(jax.random.fold_in(rng, 6), dim), (shards_of,), jnp.float32, least / len(shards), high / len(shards))
        return jnp.repeat(jnp.exp(draws), shape[dim] // shards_of).reshape((-1,) + (1,) * (len(shape) - dim - 1))

    loudness = one(*shards[0])
    for cut in shards[1:]:
        loudness = loudness * one(*cut)
    return loudness


def noise(stream_key, shape, spread, bound, pieces=(), held_as=jnp.bfloat16):
    gain = shard_levels(stream_key, shape, pieces, -0.22, 0.18) if pieces else 1.0
    entries = jax.random.normal(stream_key, shape, jnp.float32) * spread * gain
    return jnp.minimum(jnp.maximum(entries, -bound), bound).astype(held_as)


def setup_inputs(seed: int = 0) -> dict:
    key_of = jax.random.split(jax.random.key(seed), 7)
    return {
        "volt": noise(key_of[0], (NX, NY, NZ * KC), 1.0, 6.0, ((0, 16), (1, 2)), jnp.float32),
        "drive": noise(key_of[1], (NX, NY, NZ * KC), 1.0, 6.0, ((0, 16), (1, 2)), jnp.float32),
        "region": with_ends(jax.random.randint(key_of[2], (NX, NY, NZ), 0, REGIONS), jax.random.fold_in(key_of[2], 1), 0, REGIONS - 1).astype(jnp.int32),
        "diode_mask": with_ends((jax.random.randint(key_of[3], (NX, NY, NZ), 0, 4) < 1).astype(jnp.int32), jax.random.fold_in(key_of[3], 1), 0, 1),
        "sigma_table": jnp.clip(jnp.exp(jax.random.uniform(key_of[4], (REGIONS,), jnp.float32, math.log(0.3), math.log(3.0))), 0.3, 3.0),
        "cap_table": jnp.clip(jnp.exp(jax.random.uniform(key_of[5], (REGIONS,), jnp.float32, math.log(0.1), math.log(1.0))), 0.1, 1.0),
    }


base_freq = 0.1
norm_eps = 1e-06

def cut_slab(array, first_idx, last_idx, along):
    return lax.slice_in_dim(array, first_idx, last_idx, axis=along)

def harmonic_mean(left, right):
    return 2.0 * left * right / (left + right)

def open_terms(volt_field, conduct, along):
    cell_count = volt_field.shape[along]
    widths = [(0, 0)] * volt_field.ndim
    widths[along] = (1, 1)
    padded_volt = jnp.pad(volt_field, widths)
    padded_cond = jnp.pad(conduct, widths)
    face_flux = harmonic_mean(cut_slab(padded_cond, 0, cell_count + 1, along), cut_slab(padded_cond, 1, cell_count + 2, along)) * (cut_slab(padded_volt, 1, cell_count + 2, along) - cut_slab(padded_volt, 0, cell_count + 1, along))
    return cut_slab(face_flux, 0, cell_count, along) - cut_slab(face_flux, 1, cell_count + 1, along)

def time_derivative(coefs):
    half_count = coefs.shape[-1] // 2
    orders = base_freq * jnp.arange(1, half_count + 1, dtype=jnp.float32)
    return jnp.concatenate([orders * coefs[..., half_count:], -orders * coefs[..., :half_count]], axis=-1)

def spectral_tables(harmonics, samples):
    orders = jnp.arange(1, harmonics + 1, dtype=jnp.float32)
    times = 2.0 * math.pi * jnp.arange(samples, dtype=jnp.float32) / samples
    angles = orders[:, None] * times[None, :]
    synthesis = jnp.concatenate([jnp.cos(angles), jnp.sin(angles)], axis=0)
    analysis = synthesis.T * (2.0 / samples)
    return (synthesis, analysis)

def nonlinear_row(volt_row, diode_row, synthesis, analysis):
    coef_count = volt_row.shape[-1]
    flat = volt_row.reshape(-1, coef_count)
    cell_count = flat.shape[0]
    samples = jnp.dot(flat, synthesis, precision=lax.Precision.HIGHEST, preferred_element_type=jnp.float32)
    current = jax.nn.softplus(2.0 * samples) * 0.5
    charge = jnp.tanh(samples) * 0.5
    projected = jnp.dot(jnp.concatenate([current, charge], axis=0), analysis, precision=lax.Precision.HIGHEST, preferred_element_type=jnp.float32)
    combined = projected[:cell_count] + time_derivative(projected[cell_count:])
    return combined.reshape(volt_row.shape) * diode_row[..., None]

def reference(volt, drive, region, diode_mask, sigma_table, cap_table):
    conduct = jnp.take(sigma_table, region)[..., None]
    capacity = jnp.take(cap_table, region)[..., None]
    volt_field = volt.reshape(NX, NY, NZ, KC)
    drive_field = drive.reshape(NX, NY, NZ, KC)
    diode_field = diode_mask.astype(jnp.float32)
    synthesis, analysis = spectral_tables(H, S)

    def picker(array, row_index):
        return lax.dynamic_index_in_dim(array, row_index, 0, keepdims=False)

    def one_row(row_index):
        prev_row = (row_index - 1 + NX) % NX
        next_row = (row_index + 1) % NX
        volt_here = picker(volt_field, row_index)
        cond_here = picker(conduct, row_index)
        volt_prev = picker(volt_field, prev_row)
        cond_prev = picker(conduct, prev_row)
        volt_next = picker(volt_field, next_row)
        cond_next = picker(conduct, next_row)
        below_flux = harmonic_mean(cond_prev, cond_here) * (volt_here - volt_prev)
        above_flux = harmonic_mean(cond_here, cond_next) * (volt_next - volt_here)
        row_terms = below_flux - above_flux
        col_terms = open_terms(volt_here, cond_here, 0)
        depth_terms = open_terms(volt_here, cond_here, 1)
        diode_part = nonlinear_row(volt_here, picker(diode_field, row_index), synthesis, analysis)
        residual = row_terms + col_terms + depth_terms + picker(capacity, row_index) * time_derivative(volt_here) + diode_part - picker(drive_field, row_index)
        return (residual, lax.optimization_barrier(jnp.sum(residual * residual, axis=(0, 1))))
    residual, row_squares = lax.map(one_row, jnp.arange(NX, dtype=jnp.int32))
    summed = lax.optimization_barrier(jnp.sum(row_squares, axis=0))
    norms_out = jnp.sqrt(summed / (NX * NY * NZ) + norm_eps)
    return (residual.reshape(NX, NY, NZ * KC), norms_out)
```

```python
import functools
import math

import jax
import jax.numpy as jnp
import numpy as np
from jax import lax
from jax.experimental import pallas as pl
from jax.experimental.pallas import tpu as pltpu
from jax.sharding import PartitionSpec as P

NZ = 32
H = 32
KC = 64
S = 256
LANES = 128
TILES = NZ * KC // LANES
CHUNK = 4
PIECES = 4

base_freq = 0.1
norm_eps = 1e-06
MESH = pl.DeviceIdType.MESH


def tables():
    orders = np.arange(1, H + 1, dtype=np.float64)
    angles = orders[:, None] * (2.0 * math.pi * np.arange(S) / S)[None, :]
    synthesis = np.concatenate([np.cos(angles), np.sin(angles)], axis=0)
    analysis = synthesis.T * (2.0 / S)
    derived = np.concatenate(
        [base_freq * orders * analysis[:, H:], -base_freq * orders * analysis[:, :H]], axis=1
    )

    def pair(table):
        zeros = np.zeros_like(table)
        return np.block([[table, zeros], [zeros, table]])

    def split(table):
        high = table.astype(jnp.bfloat16)
        low = (table - high.astype(np.float64)).astype(jnp.bfloat16)
        return high, low

    high, _ = split(pair(synthesis))
    forward = np.concatenate([high, high], axis=0)
    high, low = split(0.5 * np.concatenate([pair(analysis), pair(derived)], axis=0))
    return jnp.asarray(forward), jnp.asarray(np.concatenate([high, low], axis=1))


def lookup(region, table, count):
    value = jnp.where(region == 0, table[0], 0.0)
    for r in range(1, count):
        value = jnp.where(region == r, table[r], value)
    return value


def harmonic_mean(left, right):
    return 2.0 * left * right / (left + right)


def spread(cells, tile, lane, base=0):
    index = base + 2 * tile + (lane >= KC).astype(jnp.int32)
    return jnp.take_along_axis(cells, index, axis=1, mode="promise_in_bounds")


def square_sum(value):
    return jnp.sum((value * value).reshape(-1, 8, LANES), axis=0)


def kernel(
    nx, ny, rows, cols, regions,
    volt_hbm, drive_hbm, region_hbm, mask_hbm, sigma_hbm, cap_hbm, forward_hbm, back_hbm,
    out_ref, norm_ref,
    volt_buf, drive_buf, region_buf, mask_buf, end_region, side_buf, side_region,
    sigma_ref, cap_ref, forward_ref, back_ref, cell_buf, turn_buf, flux_buf, acc_ref, got,
    volt_sem, drive_sem, misc_sem, row_send, row_recv, side_send, side_recv, norm_send, norm_recv,
):
    me_x, me_y = lax.axis_index("gx"), lax.axis_index("gy")
    up, down = lax.rem(me_x + 1, nx), lax.rem(me_x + nx - 1, nx)
    has_left, has_right = me_y > 0, me_y < ny - 1
    barrier = pltpu.get_barrier_semaphore()

    for dx in range(nx):
        for dy in range(ny):
            if dx or dy:
                peer = (lax.rem(me_x + dx, nx), lax.rem(me_y + dy, ny))
                pl.semaphore_signal(barrier, inc=1, device_id=peer, device_id_type=MESH)

    def volt_copy(row):
        return pltpu.make_async_copy(volt_hbm.at[row], volt_buf.at[row + 1], volt_sem.at[row])

    def drive_copy(row):
        return pltpu.make_async_copy(drive_hbm.at[row], drive_buf.at[row], drive_sem.at[row])

    misc = [
        pltpu.make_async_copy(region_hbm, region_buf, misc_sem.at[0]),
        pltpu.make_async_copy(mask_hbm, mask_buf, misc_sem.at[1]),
        pltpu.make_async_copy(sigma_hbm, sigma_ref, misc_sem.at[2]),
        pltpu.make_async_copy(cap_hbm, cap_ref, misc_sem.at[3]),
        pltpu.make_async_copy(forward_hbm, forward_ref, misc_sem.at[4]),
        pltpu.make_async_copy(back_hbm, back_ref, misc_sem.at[5]),
    ]
    volt_copy(rows - 1).start()
    volt_copy(0).start()
    for c in misc:
        c.start()
    for row in range(rows):
        if 0 < row < rows - 1:
            volt_copy(row).start()
        drive_copy(row).start()

    def remote(source, target, send, recv, axis, peer):
        return pltpu.make_async_remote_copy(
            src_ref=source, dst_ref=target, send_sem=send, recv_sem=recv,
            device_id={axis: peer}, device_id_type=MESH,
        )

    row_copies = [
        remote(region_buf.at[rows - 1], end_region.at[0], row_send.at[0], row_recv.at[0], "gx", up),
        remote(region_buf.at[0], end_region.at[1], row_send.at[1], row_recv.at[1], "gx", down),
    ]
    piece = TILES // PIECES * LANES
    for p in range(PIECES):
        lanes = pl.ds(p * piece, piece)
        for k, (source, target, peer) in enumerate(((rows, 0, up), (1, rows + 1, down))):
            n = 2 + 2 * p + k
            row_copies.append(remote(
                volt_buf.at[source, :, lanes], volt_buf.at[target, :, lanes],
                row_send.at[n], row_recv.at[n], "gx", peer,
            ))
    to_right = [
        remote(volt_hbm.at[:, pl.ds(cols - 1, 1), :], side_buf.at[0], side_send.at[0],
               side_recv.at[0], "gy", me_y + 1),
        remote(region_buf, side_region.at[0], side_send.at[1], side_recv.at[1], "gy", me_y + 1),
    ]
    to_left = [
        remote(volt_hbm.at[:, pl.ds(0, 1), :], side_buf.at[1], side_send.at[2],
               side_recv.at[2], "gy", me_y - 1),
        remote(region_buf, side_region.at[1], side_send.at[3], side_recv.at[3], "gy", me_y - 1),
    ]

    volt_copy(rows - 1).wait()
    volt_copy(0).wait()
    misc[0].wait()
    pl.semaphore_wait(barrier, nx * ny - 1)
    for c in row_copies:
        c.start()

    @pl.when(has_right)
    def _():
        for c in to_right:
            c.start()

    @pl.when(has_left)
    def _():
        for c in to_left:
            c.start()

    for c in misc[1:4]:
        c.wait()
    turn_buf[...] = jnp.zeros_like(turn_buf)

    for i in range(rows):
        turn_buf[i, :NZ, :cols] = lookup(region_buf[i], sigma_ref, regions)
        turn_buf[i, NZ : 2 * NZ, :cols] = lookup(region_buf[i], cap_ref, regions)
        turn_buf[i, 2 * NZ : 3 * NZ, :cols] = mask_buf[i].astype(jnp.float32)
    for i in range(rows):
        cell_buf[i] = turn_buf[i].T[:cols]
    flux_buf[...] = jnp.zeros_like(flux_buf)
    acc_ref[...] = jnp.zeros_like(acc_ref)
    misc[4].wait()
    misc[5].wait()

    lane = lax.broadcasted_iota(jnp.int32, (cols, LANES), 1)
    col = lax.broadcasted_iota(jnp.int32, (cols, LANES), 0)
    first = lane < KC
    half = lane % KC
    order = base_freq * (half % H + 1).astype(jnp.float32)
    order = jnp.where(half < H, order, -order)
    swap = lane ^ H

    def row_step(i, _):
        @pl.when(i < rows - 2)
        def _():
            volt_copy(i + 1).wait()

        drive_copy(i).wait()
        cells = cell_buf[i]
        after = jnp.minimum(i + 1, rows - 1)
        g_high = harmonic_mean(cells, cell_buf[after])
        g_col = harmonic_mean(cells, pltpu.roll(cells, cols - 1, 0))
        g_col = jnp.where(col == cols - 1, 0.0, g_col)
        g_depth = harmonic_mean(cells, pltpu.roll(cells, LANES - 1, 1))
        g_depth = jnp.where(lane < NZ - 1, g_depth, 0.0)
        prev_flux = None
        total = jnp.zeros((8, LANES), jnp.float32)
        for start in range(0, TILES, CHUNK):
            xs = []
            for t in range(start, start + CHUNK):
                v = volt_buf[i + 1, :, t * LANES : (t + 1) * LANES]
                high = v.astype(jnp.bfloat16)
                low = (v - high.astype(jnp.float32)).astype(jnp.bfloat16)
                xs.append(jnp.concatenate([high, low], axis=1))
            samples = jnp.dot(
                jnp.concatenate(xs, axis=0), forward_ref[...], preferred_element_type=jnp.float32
            )
            size = jnp.abs(samples)
            small = jnp.exp2(size * (-2.0 / math.log(2.0)) - 1.0)
            even = (size + jnp.log(0.5 + small)).astype(jnp.bfloat16)
            charge = jnp.tanh(samples.astype(jnp.bfloat16))
            projected = jnp.dot(
                jnp.concatenate([even, charge], axis=1), back_ref[...],
                preferred_element_type=jnp.float32,
            )
            projected = projected[:, :LANES] + projected[:, LANES:]
            for t in range(start, start + CHUNK):
                at = slice(t * LANES, (t + 1) * LANES)
                v = volt_buf[i + 1, :, at]
                flux = spread(g_high, t, lane) * (volt_buf[after + 1, :, at] - v)
                value = flux_buf[:, at] - flux
                flux_buf[:, at] = flux
                flux = spread(g_col, t, lane) * (pltpu.roll(v, cols - 1, 0) - v)
                value += pltpu.roll(flux, 1, 0) - flux
                ahead = volt_buf[i + 1, :, (t + 1) * LANES : (t + 2) * LANES] if t + 1 < TILES else v
                deep = pltpu.roll(jnp.where(first, ahead, v), KC, 1)
                flux = spread(g_depth, t, lane) * (deep - v)
                flux_r = pltpu.roll(flux, KC, 1)
                before = jnp.zeros_like(flux_r) if prev_flux is None else prev_flux
                value += jnp.where(first, before, flux_r) - flux
                prev_flux = flux_r
                swapped = jnp.take_along_axis(v, swap, axis=1, mode="promise_in_bounds")
                value += spread(cells, t, lane, NZ) * (order * swapped)
                rows_of = slice((t - start) * cols, (t - start + 1) * cols)
                value += spread(cells, t, lane, 2 * NZ) * (projected[rows_of] + 0.5 * v)
                value -= drive_buf[i, :, at]
                out_ref[i, :, at] = value
                total += square_sum(value[8 : cols - 8])
        inside = jnp.logical_and(i > 0, i < rows - 1)
        acc_ref[...] += jnp.where(inside, total, 0.0)
        return 0

    lax.fori_loop(0, rows, row_step, 0)

    lane8, sub8 = lane[:8], col[:8]

    def side_step(side):
        edge = 0 if side == 0 else cols - 8
        line = 0 if side == 0 else 7
        there = cols - 1 if side == 0 else 0

        def step(i, _):
            turn_buf[i, :NZ, :cols] = lookup(side_region[side, i], sigma_ref, regions)
            near = jnp.broadcast_to(turn_buf[i].T[there : there + 1], (8, LANES))
            g = harmonic_mean(cell_buf[i, edge : edge + 8], near)
            g = jnp.where(sub8 == line, g, 0.0)
            for t in range(TILES):
                at = slice(t * LANES, (t + 1) * LANES)
                v = volt_buf[i + 1, edge : edge + 8, at]
                far = jnp.broadcast_to(side_buf[side, i, :, at], (8, LANES))
                out_ref[i, edge : edge + 8, at] += spread(g, t, lane8) * (v - far)
            return 0

        return step

    @pl.when(has_left)
    def _():
        for c in to_right:
            c.wait_recv()
        lax.fori_loop(0, rows, side_step(0), 0)

    @pl.when(has_right)
    def _():
        for c in to_left:
            c.wait_recv()
        lax.fori_loop(0, rows, side_step(1), 0)

    def edge_squares(i, total):
        for t in range(TILES):
            at = slice(t * LANES, (t + 1) * LANES)
            total += square_sum(out_ref[i, :8, at]) + square_sum(out_ref[i, cols - 8 :, at])
        return total

    total = lax.fori_loop(1, rows - 1, edge_squares, acc_ref[...])

    row_copies[0].wait_recv()
    row_copies[1].wait_recv()
    ends = []
    for k in range(2):
        turn_buf[k, :NZ, :cols] = lookup(end_region[k], sigma_ref, regions)
    for k, i in ((0, 0), (1, rows - 1)):
        ends.append(harmonic_mean(cell_buf[i], turn_buf[k].T[:cols]))
    for p in range(PIECES):
        for k, i in ((0, 0), (1, rows - 1)):
            row_copies[2 + 2 * p + k].wait_recv()
            for t in range(p * TILES // PIECES, (p + 1) * TILES // PIECES):
                at = slice(t * LANES, (t + 1) * LANES)
                v = volt_buf[i + 1, :, at]
                value = out_ref[i, :, at]
                value += spread(ends[k], t, lane) * (v - volt_buf[k * (rows + 1), :, at])
                out_ref[i, :, at] = value
                total += square_sum(value)

    here = me_x * ny + me_y
    got[here] = jnp.sum(total, axis=0, keepdims=True)

    for c in row_copies:
        c.wait_send()

    @pl.when(has_right)
    def _():
        for c in to_right:
            c.wait_send()

    @pl.when(has_left)
    def _():
        for c in to_left:
            c.wait_send()

    def norm_copy(dx, dy, sent):
        x, y = lax.rem(me_x + dx, nx), lax.rem(me_y + dy, ny)
        slot = here if sent else x * ny + y
        return pltpu.make_async_remote_copy(
            src_ref=got.at[here], dst_ref=got.at[slot],
            send_sem=norm_send.at[x * ny + y], recv_sem=norm_recv.at[slot],
            device_id=(x, y), device_id_type=MESH,
        )

    peers = [(dx, dy) for dx in range(nx) for dy in range(ny) if dx or dy]
    for dx, dy in peers:
        norm_copy(dx, dy, True).start()
    for dx, dy in peers:
        norm_copy(dx, dy, False).wait_recv()
    value = jnp.broadcast_to(jnp.sum(got[...], axis=0), (8, LANES))
    value = value + pltpu.roll(value, KC, 1)
    value = jnp.sqrt(value / float(rows * cols * NZ * nx * ny) + norm_eps)
    norm_ref[...] = value[:1, :KC]
    for dx, dy in peers:
        norm_copy(dx, dy, True).wait_send()


def write_kernel(residual, norms, residual_out, norms_out, sems):
    copies = [
        pltpu.make_async_copy(residual, residual_out, sems.at[0]),
        pltpu.make_async_copy(norms, norms_out, sems.at[1]),
    ]
    for c in copies:
        c.start()
    for c in copies:
        c.wait()


def body(volt, drive, region, diode_mask, sigma_table, cap_table):
    rows, cols, width = volt.shape
    regions = sigma_table.shape[0]
    nx, ny = lax.axis_size("gx"), lax.axis_size("gy")
    n = nx * ny
    region = jnp.transpose(region, (0, 2, 1))
    diode_mask = jnp.transpose(diode_mask, (0, 2, 1))
    forward, back = tables()
    hbm = pl.BlockSpec(memory_space=pltpu.HBM)
    vmem = pl.BlockSpec(memory_space=pltpu.VMEM)
    dma = pltpu.SemaphoreType.DMA
    residual, norms = pl.pallas_call(
        functools.partial(kernel, nx, ny, rows, cols, regions),
        out_shape=(
            pltpu.VMEM(volt.shape, jnp.float32),
            pltpu.VMEM((1, KC), jnp.float32),
        ),
        in_specs=[hbm] * 8,
        out_specs=(vmem, vmem),
        scratch_shapes=[
            pltpu.VMEM((rows + 2, cols, width), jnp.float32),
            pltpu.VMEM((rows, cols, width), jnp.float32),
            pltpu.VMEM((rows, NZ, cols), jnp.int32),
            pltpu.VMEM((rows, NZ, cols), jnp.int32),
            pltpu.VMEM((2, NZ, cols), jnp.int32),
            pltpu.VMEM((2, rows, 1, width), jnp.float32),
            pltpu.VMEM((2, rows, NZ, cols), jnp.int32),
            pltpu.SMEM((regions,), jnp.float32),
            pltpu.SMEM((regions,), jnp.float32),
            pltpu.VMEM(forward.shape, jnp.bfloat16),
            pltpu.VMEM(back.shape, jnp.bfloat16),
            pltpu.VMEM((rows, cols, LANES), jnp.float32),
            pltpu.VMEM((rows, LANES, LANES), jnp.float32),
            pltpu.VMEM((cols, width), jnp.float32),
            pltpu.VMEM((8, LANES), jnp.float32),
            pltpu.VMEM((n, 1, LANES), jnp.float32),
            dma((rows,)),
            dma((rows,)),
            dma((6,)),
            dma((2 + 2 * PIECES,)),
            dma((2 + 2 * PIECES,)),
            dma((4,)),
            dma((4,)),
            dma((n,)),
            dma((n,)),
        ],
        compiler_params=pltpu.CompilerParams(
            collective_id=0, has_side_effects=True, vmem_limit_bytes=50 * 2**20
        ),
        name="balance",
    )(volt, drive, region, diode_mask, sigma_table, cap_table, forward, back)
    residual, norms = pl.pallas_call(
        write_kernel,
        out_shape=(
            jax.ShapeDtypeStruct(volt.shape, jnp.float32),
            jax.ShapeDtypeStruct((1, KC), jnp.float32),
        ),
        in_specs=[vmem, vmem],
        out_specs=(hbm, hbm),
        scratch_shapes=[dma((2,))],
        compiler_params=pltpu.CompilerParams(vmem_limit_bytes=2**20),
        name="write",
    )(residual, norms)
    return residual, norms.reshape(KC)


def solution(mesh):
    return jax.shard_map(
        body,
        mesh=mesh,
        in_specs=(
            P("gx", "gy", None),
            P("gx", "gy", None),
            P("gx", "gy", None),
            P("gx", "gy", None),
            P(),
            P(),
        ),
        out_specs=(P("gx", "gy", None), P()),
        check_vma=False,
    )
```

```python
import functools
import math

import jax
import jax.numpy as jnp
import numpy as np
from jax import lax
from jax.experimental import pallas as pl
from jax.experimental.pallas import tpu as pltpu
from jax.sharding import PartitionSpec as P

NZ = 32
H = 32
KC = 64
S = 256
LANES = 128
TILES = NZ * KC // LANES
CHUNK = 8
PIECES = 2
SEND = 0

base_freq = 0.1
norm_eps = 1e-06
MESH = pl.DeviceIdType.MESH


def tables():
    orders = np.arange(1, H + 1, dtype=np.float64)
    angles = orders[:, None] * (2.0 * math.pi * np.arange(S) / S)[None, :]
    synthesis = np.concatenate([np.cos(angles), np.sin(angles)], axis=0)
    analysis = synthesis.T * (2.0 / S)
    derived = np.concatenate(
        [base_freq * orders * analysis[:, H:], -base_freq * orders * analysis[:, :H]], axis=1
    )

    def pair(table):
        zeros = np.zeros_like(table)
        return np.block([[table, zeros], [zeros, table]])

    def split(table):
        high = table.astype(jnp.bfloat16)
        low = (table - high.astype(np.float64)).astype(jnp.bfloat16)
        return high, low

    high, _ = split(pair(synthesis))
    forward = np.concatenate([high, high], axis=0)
    high, low = split(0.5 * np.concatenate([pair(analysis), pair(derived)], axis=0))
    back = np.concatenate([high, low], axis=1)
    wide = CHUNK * LANES
    place = np.zeros((4, NZ, TILES // CHUNK, 2, wide), jnp.bfloat16)
    for z in range(NZ):
        chunk, at = divmod(z * KC, wide)
        for k in range(4):
            place[k, z, chunk, k // 2, at : at + KC] = 1
    return jnp.asarray(forward), jnp.asarray(back), jnp.asarray(place.reshape(4 * NZ, -1))


def lookup(region, table, count):
    value = jnp.where(region == 0, table[0], 0.0)
    for r in range(1, count):
        value = jnp.where(region == r, table[r], value)
    return value


def harmonic_mean(left, right):
    return 2.0 * left * right / (left + right)


def packed(a, b):
    parts = []
    for g in (a, b):
        high = g.astype(jnp.bfloat16).astype(jnp.float32)
        parts += [high, g - high]
    return jnp.concatenate(parts, axis=0).T.astype(jnp.bfloat16)


def fold(value):
    return jnp.sum(value.reshape(-1, 8, LANES), axis=0)


def kernel(
    nx, ny, rows, cols, regions,
    volt_hbm, drive_hbm, region_hbm, mask_hbm, sigma_hbm, cap_hbm, forward_hbm, back_hbm, place_hbm,
    out_ref, norm_ref,
    volt_buf, drive_buf, region_buf, mask_buf, end_region, side_buf, side_region,
    sigma_ref, cap_ref, forward_ref, back_ref, place_ref, cond_buf, edge_buf, flux_buf, line_buf,
    acc_ref, got,
    volt_sem, drive_sem, misc_sem, row_send, row_recv, side_send, side_recv, norm_send, norm_recv,
):
    me_x, me_y = lax.axis_index("gx"), lax.axis_index("gy")
    up, down = lax.rem(me_x + 1, nx), lax.rem(me_x + nx - 1, nx)
    has_left, has_right = me_y > 0, me_y < ny - 1
    barrier = pltpu.get_barrier_semaphore()

    for dx in range(nx):
        for dy in range(ny):
            if dx or dy:
                peer = (lax.rem(me_x + dx, nx), lax.rem(me_y + dy, ny))
                pl.semaphore_signal(barrier, inc=1, device_id=peer, device_id_type=MESH)

    def volt_copy(row):
        return pltpu.make_async_copy(volt_hbm.at[row], volt_buf.at[row + 1], volt_sem.at[row])

    def drive_copy(row):
        return pltpu.make_async_copy(drive_hbm.at[row], drive_buf.at[row], drive_sem.at[row])

    misc = [
        pltpu.make_async_copy(region_hbm, region_buf, misc_sem.at[0]),
        pltpu.make_async_copy(mask_hbm, mask_buf, misc_sem.at[1]),
        pltpu.make_async_copy(sigma_hbm, sigma_ref, misc_sem.at[2]),
        pltpu.make_async_copy(cap_hbm, cap_ref, misc_sem.at[3]),
        pltpu.make_async_copy(forward_hbm, forward_ref, misc_sem.at[4]),
        pltpu.make_async_copy(back_hbm, back_ref, misc_sem.at[5]),
        pltpu.make_async_copy(place_hbm, place_ref, misc_sem.at[6]),
    ]
    volt_copy(0).start()
    volt_copy(1).start()
    for c in misc:
        c.start()
    drive_copy(0).start()
    volt_copy(rows - 1).start()
    for row in range(2, rows - 1):
        volt_copy(row).start()
    for row in range(1, rows):
        drive_copy(row).start()

    def remote(source, target, send, recv, axis, peer):
        return pltpu.make_async_remote_copy(
            src_ref=source, dst_ref=target, send_sem=send, recv_sem=recv,
            device_id={axis: peer}, device_id_type=MESH,
        )

    row_copies = [
        remote(region_buf.at[rows - 1], end_region.at[0], row_send.at[0], row_recv.at[0], "gx", up),
        remote(region_buf.at[0], end_region.at[1], row_send.at[1], row_recv.at[1], "gx", down),
    ]
    piece = TILES // PIECES * LANES
    for p in range(PIECES):
        lanes = pl.ds(p * piece, piece)
        for k, (source, target, peer) in enumerate(((rows, 0, up), (1, rows + 1, down))):
            n = 2 + 2 * p + k
            row_copies.append(remote(
                volt_buf.at[source, :, lanes], volt_buf.at[target, :, lanes],
                row_send.at[n], row_recv.at[n], "gx", peer,
            ))
    to_right = [
        remote(volt_buf.at[pl.ds(1, rows), pl.ds(cols - 1, 1), :], side_buf.at[0], side_send.at[0],
               side_recv.at[0], "gy", me_y + 1),
        remote(region_buf, side_region.at[0], side_send.at[1], side_recv.at[1], "gy", me_y + 1),
    ]
    to_left = [
        remote(volt_buf.at[pl.ds(1, rows), pl.ds(0, 1), :], side_buf.at[1], side_send.at[2],
               side_recv.at[2], "gy", me_y - 1),
        remote(region_buf, side_region.at[1], side_send.at[3], side_recv.at[3], "gy", me_y - 1),
    ]

    def send():
        for row in range(2, rows):
            volt_copy(row).wait()
        pl.semaphore_wait(barrier, nx * ny - 1)
        for c in row_copies:
            c.start()

        @pl.when(has_right)
        def _():
            for c in to_right:
                c.start()

        @pl.when(has_left)
        def _():
            for c in to_left:
                c.start()

    volt_copy(0).wait()
    volt_copy(1).wait()
    for c in misc[:4]:
        c.wait()
    lane = lax.broadcasted_iota(jnp.int32, (cols, LANES), 1)
    first = lane < KC
    half = lane % KC
    order = base_freq * (half % H + 1).astype(jnp.float32)
    order = jnp.where(half < H, order, -order)
    swap = lane ^ H
    lane_t = lane[:NZ]
    depth_t = lax.broadcasted_iota(jnp.int32, (NZ, LANES), 0)

    def padded(table):
        rest = jnp.ones((NZ, LANES - cols), jnp.float32)
        return jnp.concatenate([table, rest], axis=1)

    for i in range(rows):
        cond_buf[i] = padded(lookup(region_buf[i], sigma_ref, regions))
    for i in range(rows):
        cond = cond_buf[i]
        g_high = harmonic_mean(cond, cond_buf[min(i + 1, rows - 1)])
        g_col = harmonic_mean(cond, pltpu.roll(cond, LANES - 1, 1))
        g_col = jnp.where(lane_t == cols - 1, 0.0, g_col)
        g_deep = harmonic_mean(cond, pltpu.roll(cond, NZ - 1, 0))
        g_deep = jnp.where(depth_t < NZ - 1, g_deep, 0.0)
        cap = padded(lookup(region_buf[i], cap_ref, regions))
        diode = padded(mask_buf[i].astype(jnp.float32))
        edge_buf[i, 0] = packed(g_high, g_col)[:cols]
        edge_buf[i, 1] = packed(g_deep, cap)[:cols]
        edge_buf[i, 2] = packed(diode, diode)[:cols]
    flux_buf[...] = jnp.zeros_like(flux_buf)
    acc_ref[...] = jnp.zeros_like(acc_ref)
    for c in misc[4:]:
        c.wait()
    wide = CHUNK * LANES

    def placed(edges, start, count=2):
        at = start * LANES * 2
        table = place_ref[:, at : at + count * wide]
        return jnp.dot(edges, table, preferred_element_type=jnp.float32)

    def row_step(i, _):
        pl.when(i == SEND)(send)
        drive_copy(i).wait()
        after = jnp.minimum(i + 2, rows)
        before = None
        total = jnp.zeros((8, LANES), jnp.float32)
        for start in range(0, TILES, CHUNK):
            xs = []
            for t in range(start, start + CHUNK):
                v = volt_buf[i + 1, :, t * LANES : (t + 1) * LANES]
                high = v.astype(jnp.bfloat16)
                low = (v - high.astype(jnp.float32)).astype(jnp.bfloat16)
                xs.append(jnp.concatenate([high, low], axis=1))
            samples = jnp.dot(
                jnp.concatenate(xs, axis=0), forward_ref[...], preferred_element_type=jnp.float32
            )
            size = jnp.abs(samples)
            small = jnp.exp2(size * (-2.0 / math.log(2.0)) - 1.0)
            even = (size + jnp.log(0.5 + small)).astype(jnp.bfloat16)
            charge = jnp.tanh(samples.astype(jnp.bfloat16))
            projected = jnp.dot(
                jnp.concatenate([even, charge], axis=1), back_ref[...],
                preferred_element_type=jnp.float32,
            )
            projected = projected[:, :LANES] + projected[:, LANES:]
            pairs = placed(edge_buf[i, :2].reshape(2 * cols, LANES), start)
            diodes = placed(edge_buf[i, 2], start, 1)
            for t in range(start, start + CHUNK):
                at = slice(t * LANES, (t + 1) * LANES)
                one = slice((t - start) * LANES, (t - start + 1) * LANES)
                two = slice(wide + (t - start) * LANES, wide + (t - start + 1) * LANES)
                v = volt_buf[i + 1, :, at]
                flux = pairs[:cols, one] * (volt_buf[after, :, at] - v)
                value = flux_buf[:, at] - flux
                flux_buf[:, at] = flux
                flux = pairs[:cols, two] * (pltpu.roll(v, cols - 1, 0) - v)
                value += pltpu.roll(flux, 1, 0) - flux
                ahead = volt_buf[i + 1, :, (t + 1) * LANES : (t + 2) * LANES] if t + 1 < TILES else v
                deep = pltpu.roll(jnp.where(first, ahead, v), KC, 1)
                flux = pairs[cols:, one] * (deep - v)
                flux_r = pltpu.roll(flux, KC, 1)
                value += jnp.where(first, jnp.zeros_like(flux_r) if before is None else before, flux_r)
                value -= flux
                before = flux_r
                swapped = jnp.take_along_axis(v, swap, axis=1, mode="promise_in_bounds")
                value += pairs[cols:, two] * (order * swapped)
                rows_of = slice((t - start) * cols, (t - start + 1) * cols)
                value += diodes[:, one] * (projected[rows_of] + 0.5 * v)
                value -= drive_buf[i, :, at]
                out_ref[i, :, at] = value
                total += fold(value * value)
        acc_ref[...] += total
        return 0

    lax.fori_loop(0, rows, row_step, 0)

    sub8 = lax.broadcasted_iota(jnp.int32, (8, LANES), 0)

    def side(k, copies):
        for c in copies:
            c.wait_recv()
        mine, theirs = (0, cols - 1) if k == 0 else (cols - 1, 0)
        edge, line = mine // 8 * 8, mine % 8
        g = jnp.zeros((NZ, LANES), jnp.float32)
        for i in range(rows):
            far = padded(lookup(side_region[k, i], sigma_ref, regions))
            far = pltpu.roll(far, (i - theirs) % LANES, 1)
            near = pltpu.roll(cond_buf[i], (i - mine) % LANES, 1)
            g = jnp.where(lane_t == i, harmonic_mean(near, far), g)
        edges = packed(g, g)[:8]
        for start in range(0, TILES, CHUNK):
            line_buf[:, start * LANES : (start + CHUNK) * LANES] = placed(edges, start, 1)
        total = jnp.zeros((8, LANES), jnp.float32)
        for i in range(rows):
            for t in range(TILES):
                at = slice(t * LANES, (t + 1) * LANES)
                far = jnp.broadcast_to(side_buf[k, i, :, at], (8, LANES))
                g = jnp.broadcast_to(line_buf[i : i + 1, at], (8, LANES))
                g = jnp.where(sub8 == line, g, 0.0)
                change = g * (volt_buf[i + 1, edge : edge + 8, at] - far)
                old = out_ref[i, edge : edge + 8, at]
                out_ref[i, edge : edge + 8, at] = old + change
                total += change * (2.0 * old + change)
        acc_ref[...] += total

    pl.when(has_left)(lambda: side(0, to_right))
    pl.when(has_right)(lambda: side(1, to_left))

    row_copies[0].wait_recv()
    row_copies[1].wait_recv()
    g_low, g_high = (
        harmonic_mean(cond_buf[i], padded(lookup(end_region[k], sigma_ref, regions)))
        for k, i in ((0, 0), (1, rows - 1))
    )
    edges = packed(g_low, g_high)[:cols]
    total = acc_ref[...]
    for start in range(0, TILES, CHUNK):
        if start % (TILES // PIECES) == 0:
            for k in range(2):
                row_copies[2 + 2 * (start * PIECES // TILES) + k].wait_recv()
        ends = placed(edges, start)
        for k, i in ((0, 0), (1, rows - 1)):
            for t in range(start, start + CHUNK):
                at = slice(t * LANES, (t + 1) * LANES)
                one = slice(k * wide + (t - start) * LANES, k * wide + (t - start + 1) * LANES)
                change = ends[:, one] * (volt_buf[i + 1, :, at] - volt_buf[k * (rows + 1), :, at])
                old = out_ref[i, :, at]
                out_ref[i, :, at] = old + change
                total += fold(change * (2.0 * old + change))

    here = me_x * ny + me_y
    got[here] = jnp.sum(total, axis=0, keepdims=True)

    for c in row_copies:
        c.wait_send()

    @pl.when(has_right)
    def _():
        for c in to_right:
            c.wait_send()

    @pl.when(has_left)
    def _():
        for c in to_left:
            c.wait_send()

    def norm_copy(dx, dy, sent):
        x, y = lax.rem(me_x + dx, nx), lax.rem(me_y + dy, ny)
        slot = here if sent else x * ny + y
        return pltpu.make_async_remote_copy(
            src_ref=got.at[here], dst_ref=got.at[slot],
            send_sem=norm_send.at[x * ny + y], recv_sem=norm_recv.at[slot],
            device_id=(x, y), device_id_type=MESH,
        )

    peers = [(dx, dy) for dx in range(nx) for dy in range(ny) if dx or dy]
    for dx, dy in peers:
        norm_copy(dx, dy, True).start()
    for dx, dy in peers:
        norm_copy(dx, dy, False).wait_recv()
    value = jnp.broadcast_to(jnp.sum(got[...], axis=0), (8, LANES))
    value = value + pltpu.roll(value, KC, 1)
    value = jnp.sqrt(value / float(rows * cols * NZ * nx * ny) + norm_eps)
    norm_ref[...] = value[:1, :KC]
    for dx, dy in peers:
        norm_copy(dx, dy, True).wait_send()


def write_kernel(residual, norms, residual_out, norms_out, sems):
    copies = [
        pltpu.make_async_copy(residual, residual_out, sems.at[0]),
        pltpu.make_async_copy(norms, norms_out, sems.at[1]),
    ]
    for c in copies:
        c.start()
    for c in copies:
        c.wait()


def body(volt, drive, region, diode_mask, sigma_table, cap_table):
    rows, cols, width = volt.shape
    regions = sigma_table.shape[0]
    nx, ny = lax.axis_size("gx"), lax.axis_size("gy")
    n = nx * ny
    region = jnp.transpose(region, (0, 2, 1))
    diode_mask = jnp.transpose(diode_mask, (0, 2, 1))
    forward, back, place = tables()
    hbm = pl.BlockSpec(memory_space=pltpu.HBM)
    vmem = pl.BlockSpec(memory_space=pltpu.VMEM)
    dma = pltpu.SemaphoreType.DMA
    residual, norms = pl.pallas_call(
        functools.partial(kernel, nx, ny, rows, cols, regions),
        out_shape=(
            pltpu.VMEM(volt.shape, jnp.float32),
            pltpu.VMEM((1, KC), jnp.float32),
        ),
        in_specs=[hbm] * 9,
        out_specs=(vmem, vmem),
        scratch_shapes=[
            pltpu.VMEM((rows + 2, cols, width), jnp.float32),
            pltpu.VMEM((rows, cols, width), jnp.float32),
            pltpu.VMEM((rows, NZ, cols), jnp.int32),
            pltpu.VMEM((rows, NZ, cols), jnp.int32),
            pltpu.VMEM((2, NZ, cols), jnp.int32),
            pltpu.VMEM((2, rows, 1, width), jnp.float32),
            pltpu.VMEM((2, rows, NZ, cols), jnp.int32),
            pltpu.SMEM((regions,), jnp.float32),
            pltpu.SMEM((regions,), jnp.float32),
            pltpu.VMEM(forward.shape, jnp.bfloat16),
            pltpu.VMEM(back.shape, jnp.bfloat16),
            pltpu.VMEM(place.shape, jnp.bfloat16),
            pltpu.VMEM((rows, NZ, LANES), jnp.float32),
            pltpu.VMEM((rows, 3, cols, LANES), jnp.bfloat16),
            pltpu.VMEM((cols, width), jnp.float32),
            pltpu.VMEM((8, width), jnp.float32),
            pltpu.VMEM((8, LANES), jnp.float32),
            pltpu.VMEM((n, 1, LANES), jnp.float32),
            dma((rows,)),
            dma((rows,)),
            dma((7,)),
            dma((2 + 2 * PIECES,)),
            dma((2 + 2 * PIECES,)),
            dma((4,)),
            dma((4,)),
            dma((n,)),
            dma((n,)),
        ],
        compiler_params=pltpu.CompilerParams(
            collective_id=0, has_side_effects=True, vmem_limit_bytes=50 * 2**20
        ),
        name="balance",
    )(volt, drive, region, diode_mask, sigma_table, cap_table, forward, back, place)
    residual, norms = pl.pallas_call(
        write_kernel,
        out_shape=(
            jax.ShapeDtypeStruct(volt.shape, jnp.float32),
            jax.ShapeDtypeStruct((1, KC), jnp.float32),
        ),
        in_specs=[vmem, vmem],
        out_specs=(hbm, hbm),
        scratch_shapes=[dma((2,))],
        compiler_params=pltpu.CompilerParams(vmem_limit_bytes=2**20),
        name="write",
    )(residual, norms)
    return residual, norms.reshape(KC)


def solution(mesh):
    return jax.shard_map(
        body,
        mesh=mesh,
        in_specs=(
            P("gx", "gy", None),
            P("gx", "gy", None),
            P("gx", "gy", None),
            P("gx", "gy", None),
            P(),
            P(),
        ),
        out_specs=(P("gx", "gy", None), P()),
        check_vma=False,
    )
```

```python
import functools
import math

import jax
import jax.numpy as jnp
import numpy as np
from jax import lax
from jax.experimental import pallas as pl
from jax.experimental.pallas import tpu as pltpu
from jax.sharding import PartitionSpec as P

NZ = 32
H = 32
KC = 64
S = 256
LANES = 128
TILES = NZ * KC // LANES
CHUNK = 16
PIECES = 1
SEND = 1

base_freq = 0.1
norm_eps = 1e-06
MESH = pl.DeviceIdType.MESH


def tables():
    orders = np.arange(1, H + 1, dtype=np.float64)
    angles = orders[:, None] * (2.0 * math.pi * np.arange(S) / S)[None, :]
    synthesis = np.concatenate([np.cos(angles), np.sin(angles)], axis=0)
    analysis = synthesis.T * (2.0 / S)
    derived = np.concatenate(
        [base_freq * orders * analysis[:, H:], -base_freq * orders * analysis[:, :H]], axis=1
    )

    def pair(table):
        zeros = np.zeros_like(table)
        return np.block([[table, zeros], [zeros, table]])

    def split(table):
        high = table.astype(jnp.bfloat16)
        low = (table - high.astype(np.float64)).astype(jnp.bfloat16)
        return high, low

    high, _ = split(pair(synthesis))
    forward = np.concatenate([high, high], axis=0)
    high, low = split(0.5 * np.concatenate([pair(analysis), pair(derived)], axis=0))
    back = np.concatenate([high, low], axis=1)
    wide = CHUNK * LANES
    place = np.zeros((4, NZ, TILES // CHUNK, 2, wide), jnp.bfloat16)
    for z in range(NZ):
        chunk, at = divmod(z * KC, wide)
        for k in range(4):
            place[k, z, chunk, k // 2, at : at + KC] = 1
    return jnp.asarray(forward), jnp.asarray(back), jnp.asarray(place.reshape(4 * NZ, -1))


def lookup(region, table, count):
    value = jnp.where(region == 0, table[0], 0.0)
    for r in range(1, count):
        value = jnp.where(region == r, table[r], value)
    return value


def harmonic_mean(left, right):
    return 2.0 * left * right / (left + right)


def packed(a, b):
    parts = []
    for g in (a, b):
        high = g.astype(jnp.bfloat16).astype(jnp.float32)
        parts += [high, g - high]
    return jnp.concatenate(parts, axis=0).T.astype(jnp.bfloat16)


def fold(value):
    return jnp.sum(value.reshape(-1, 8, LANES), axis=0)


def kernel(
    nx, ny, rows, cols, regions,
    volt_hbm, drive_hbm, region_hbm, mask_hbm, sigma_hbm, cap_hbm, forward_hbm, back_hbm, place_hbm,
    out_ref, norm_ref,
    volt_buf, drive_buf, region_buf, mask_buf, end_region, side_buf, side_region,
    sigma_ref, cap_ref, forward_ref, back_ref, place_ref, cond_buf, edge_buf, flux_buf, line_buf,
    acc_ref, got,
    volt_sem, drive_sem, misc_sem, row_send, row_recv, side_send, side_recv, norm_send, norm_recv,
):
    me_x, me_y = lax.axis_index("gx"), lax.axis_index("gy")
    up, down = lax.rem(me_x + 1, nx), lax.rem(me_x + nx - 1, nx)
    has_left, has_right = me_y > 0, me_y < ny - 1
    barrier = pltpu.get_barrier_semaphore()

    for dx in range(nx):
        for dy in range(ny):
            if dx or dy:
                peer = (lax.rem(me_x + dx, nx), lax.rem(me_y + dy, ny))
                pl.semaphore_signal(barrier, inc=1, device_id=peer, device_id_type=MESH)

    def volt_copy(row):
        return pltpu.make_async_copy(volt_hbm.at[row], volt_buf.at[row + 1], volt_sem.at[row])

    def drive_copy(row):
        return pltpu.make_async_copy(drive_hbm.at[row], drive_buf.at[row], drive_sem.at[row])

    misc = [
        pltpu.make_async_copy(region_hbm, region_buf, misc_sem.at[0]),
        pltpu.make_async_copy(mask_hbm, mask_buf, misc_sem.at[1]),
        pltpu.make_async_copy(sigma_hbm, sigma_ref, misc_sem.at[2]),
        pltpu.make_async_copy(cap_hbm, cap_ref, misc_sem.at[3]),
        pltpu.make_async_copy(forward_hbm, forward_ref, misc_sem.at[4]),
        pltpu.make_async_copy(back_hbm, back_ref, misc_sem.at[5]),
        pltpu.make_async_copy(place_hbm, place_ref, misc_sem.at[6]),
    ]
    misc[0].start()
    volt_copy(0).start()
    volt_copy(rows - 1).start()
    volt_copy(1).start()
    for c in misc[1:]:
        c.start()
    drive_copy(0).start()
    for row in range(2, rows - 1):
        volt_copy(row).start()
    for row in range(1, rows):
        drive_copy(row).start()

    def remote(source, target, send, recv, axis, peer):
        return pltpu.make_async_remote_copy(
            src_ref=source, dst_ref=target, send_sem=send, recv_sem=recv,
            device_id={axis: peer}, device_id_type=MESH,
        )

    row_copies = [
        remote(region_buf.at[rows - 1], end_region.at[0], row_send.at[0], row_recv.at[0], "gx", up),
        remote(region_buf.at[0], end_region.at[1], row_send.at[1], row_recv.at[1], "gx", down),
    ]
    piece = TILES // PIECES * LANES
    for p in range(PIECES):
        lanes = pl.ds(p * piece, piece)
        for k, (source, target, peer) in enumerate(((rows, 0, up), (1, rows + 1, down))):
            n = 2 + 2 * p + k
            row_copies.append(remote(
                volt_buf.at[source, :, lanes], volt_buf.at[target, :, lanes],
                row_send.at[n], row_recv.at[n], "gx", peer,
            ))
    to_right = [
        remote(volt_buf.at[pl.ds(1, rows), pl.ds(cols - 1, 1), :], side_buf.at[0], side_send.at[0],
               side_recv.at[0], "gy", me_y + 1),
        remote(region_buf, side_region.at[0], side_send.at[1], side_recv.at[1], "gy", me_y + 1),
    ]
    to_left = [
        remote(volt_buf.at[pl.ds(1, rows), pl.ds(0, 1), :], side_buf.at[1], side_send.at[2],
               side_recv.at[2], "gy", me_y - 1),
        remote(region_buf, side_region.at[1], side_send.at[3], side_recv.at[3], "gy", me_y - 1),
    ]

    def send():
        for row in range(2, rows - 1):
            volt_copy(row).wait()

        @pl.when(has_right)
        def _():
            for c in to_right:
                c.start()

        @pl.when(has_left)
        def _():
            for c in to_left:
                c.start()

    volt_copy(0).wait()
    volt_copy(rows - 1).wait()
    misc[0].wait()
    pl.semaphore_wait(barrier, nx * ny - 1)
    for c in row_copies:
        c.start()
    volt_copy(1).wait()
    for c in misc[1:4]:
        c.wait()
    lane = lax.broadcasted_iota(jnp.int32, (cols, LANES), 1)
    first = lane < KC
    half = lane % KC
    order = base_freq * (half % H + 1).astype(jnp.float32)
    order = jnp.where(half < H, order, -order)
    swap = lane ^ H
    lane_t = lane[:NZ]
    depth_t = lax.broadcasted_iota(jnp.int32, (NZ, LANES), 0)

    def padded(table):
        rest = jnp.ones((NZ, LANES - cols), jnp.float32)
        return jnp.concatenate([table, rest], axis=1)

    for i in range(rows):
        cond_buf[i] = padded(lookup(region_buf[i], sigma_ref, regions))
    for i in range(rows):
        cond = cond_buf[i]
        g_high = harmonic_mean(cond, cond_buf[min(i + 1, rows - 1)])
        g_col = harmonic_mean(cond, pltpu.roll(cond, LANES - 1, 1))
        g_col = jnp.where(lane_t == cols - 1, 0.0, g_col)
        g_deep = harmonic_mean(cond, pltpu.roll(cond, NZ - 1, 0))
        g_deep = jnp.where(depth_t < NZ - 1, g_deep, 0.0)
        cap = padded(lookup(region_buf[i], cap_ref, regions))
        diode = padded(mask_buf[i].astype(jnp.float32))
        edge_buf[i, 0] = packed(g_high, g_col)[:cols]
        edge_buf[i, 1] = packed(g_deep, cap)[:cols]
        edge_buf[i, 2] = packed(diode, diode)[:cols]
    flux_buf[...] = jnp.zeros_like(flux_buf)
    acc_ref[...] = jnp.zeros_like(acc_ref)
    for c in misc[4:]:
        c.wait()
    wide = CHUNK * LANES

    def placed(edges, start, count=2):
        at = start * LANES * 2
        table = place_ref[:, at : at + count * wide]
        return jnp.dot(edges, table, preferred_element_type=jnp.float32)

    def row_step(i, _):
        pl.when(i == SEND)(send)
        drive_copy(i).wait()
        after = jnp.minimum(i + 2, rows)
        before = None
        total = jnp.zeros((8, LANES), jnp.float32)
        for start in range(0, TILES, CHUNK):
            xs = []
            for t in range(start, start + CHUNK):
                v = volt_buf[i + 1, :, t * LANES : (t + 1) * LANES]
                high = v.astype(jnp.bfloat16)
                low = (v - high.astype(jnp.float32)).astype(jnp.bfloat16)
                xs.append(jnp.concatenate([high, low], axis=1))
            samples = jnp.dot(
                jnp.concatenate(xs, axis=0), forward_ref[...], preferred_element_type=jnp.float32
            )
            size = jnp.maximum(samples, -samples)
            small = jnp.exp2(size * (-2.0 / math.log(2.0)) - 1.0)
            even = (size + jnp.log(0.5 + small)).astype(jnp.bfloat16)
            charge = jnp.tanh(samples.astype(jnp.bfloat16))
            projected = jnp.dot(
                jnp.concatenate([even, charge], axis=1), back_ref[...],
                preferred_element_type=jnp.float32,
            )
            projected = projected[:, :LANES] + projected[:, LANES:]
            pairs = placed(edge_buf[i, :2].reshape(2 * cols, LANES), start)
            diodes = placed(edge_buf[i, 2], start, 1)
            for t in range(start, start + CHUNK):
                at = slice(t * LANES, (t + 1) * LANES)
                one = slice((t - start) * LANES, (t - start + 1) * LANES)
                two = slice(wide + (t - start) * LANES, wide + (t - start + 1) * LANES)
                v = volt_buf[i + 1, :, at]
                flux = pairs[:cols, one] * (volt_buf[after, :, at] - v)
                value = flux_buf[:, at] - flux
                flux_buf[:, at] = flux
                flux = pairs[:cols, two] * (pltpu.roll(v, cols - 1, 0) - v)
                value += pltpu.roll(flux, 1, 0) - flux
                ahead = volt_buf[i + 1, :, (t + 1) * LANES : (t + 2) * LANES] if t + 1 < TILES else v
                deep = pltpu.roll(jnp.where(first, ahead, v), KC, 1)
                flux = pairs[cols:, one] * (deep - v)
                flux_r = pltpu.roll(flux, KC, 1)
                value += jnp.where(first, jnp.zeros_like(flux_r) if before is None else before, flux_r)
                value -= flux
                before = flux_r
                swapped = jnp.take_along_axis(v, swap, axis=1, mode="promise_in_bounds")
                value += pairs[cols:, two] * (order * swapped)
                rows_of = slice((t - start) * cols, (t - start + 1) * cols)
                value += diodes[:, one] * (projected[rows_of] + 0.5 * v)
                value -= drive_buf[i, :, at]
                out_ref[i, :, at] = value
                total += fold(value * value)
        acc_ref[...] += total
        return 0

    lax.fori_loop(0, rows, row_step, 0)

    sub8 = lax.broadcasted_iota(jnp.int32, (8, LANES), 0)

    def side(k, copies):
        for c in copies:
            c.wait_recv()
        mine, theirs = (0, cols - 1) if k == 0 else (cols - 1, 0)
        edge, line = mine // 8 * 8, mine % 8
        near = jnp.ones((NZ, LANES), jnp.float32)
        far = jnp.zeros((NZ, LANES), jnp.int32)
        for i in range(rows):
            there = jnp.concatenate([side_region[k, i]] * (LANES // cols), axis=1)
            there = pltpu.roll(there, (i - theirs) % LANES, 1)
            here = pltpu.roll(cond_buf[i], (i - mine) % LANES, 1)
            far = jnp.where(lane_t == i, there, far)
            near = jnp.where(lane_t == i, here, near)
        g = harmonic_mean(near, lookup(far, sigma_ref, regions))
        edges = packed(g, g)[:8]
        for start in range(0, TILES, CHUNK):
            line_buf[:, start * LANES : (start + CHUNK) * LANES] = placed(edges, start, 1)
        total = jnp.zeros((8, LANES), jnp.float32)
        for i in range(rows):
            for t in range(TILES):
                at = slice(t * LANES, (t + 1) * LANES)
                far = jnp.broadcast_to(side_buf[k, i, :, at], (8, LANES))
                g = jnp.broadcast_to(line_buf[i : i + 1, at], (8, LANES))
                g = jnp.where(sub8 == line, g, 0.0)
                change = g * (volt_buf[i + 1, edge : edge + 8, at] - far)
                old = out_ref[i, edge : edge + 8, at]
                out_ref[i, edge : edge + 8, at] = old + change
                total += change * (2.0 * old + change)
        acc_ref[...] += total

    pl.when(has_left)(lambda: side(0, to_right))
    pl.when(has_right)(lambda: side(1, to_left))

    row_copies[0].wait_recv()
    row_copies[1].wait_recv()
    g_low, g_high = (
        harmonic_mean(cond_buf[i], padded(lookup(end_region[k], sigma_ref, regions)))
        for k, i in ((0, 0), (1, rows - 1))
    )
    edges = packed(g_low, g_high)[:cols]
    total = acc_ref[...]
    for start in range(0, TILES, CHUNK):
        if start % (TILES // PIECES) == 0:
            for k in range(2):
                row_copies[2 + 2 * (start * PIECES // TILES) + k].wait_recv()
        ends = placed(edges, start)
        for k, i in ((0, 0), (1, rows - 1)):
            for t in range(start, start + CHUNK):
                at = slice(t * LANES, (t + 1) * LANES)
                one = slice(k * wide + (t - start) * LANES, k * wide + (t - start + 1) * LANES)
                change = ends[:, one] * (volt_buf[i + 1, :, at] - volt_buf[k * (rows + 1), :, at])
                old = out_ref[i, :, at]
                out_ref[i, :, at] = old + change
                total += fold(change * (2.0 * old + change))

    here = me_x * ny + me_y
    got[here] = jnp.sum(total, axis=0, keepdims=True)

    for c in row_copies:
        c.wait_send()

    @pl.when(has_right)
    def _():
        for c in to_right:
            c.wait_send()

    @pl.when(has_left)
    def _():
        for c in to_left:
            c.wait_send()

    peers = [(dx, dy) for dx in range(nx) for dy in range(ny) if dx or dy]
    for dx, dy in peers:
        pltpu.make_async_remote_copy(
            src_ref=got.at[here], dst_ref=got.at[here],
            send_sem=norm_send, recv_sem=norm_recv,
            device_id=(lax.rem(me_x + dx, nx), lax.rem(me_y + dy, ny)), device_id_type=MESH,
        ).start()
    others = got.at[pl.ds(0, nx * ny - 1)]
    pltpu.make_async_copy(others, others, norm_recv).wait()
    value = jnp.broadcast_to(jnp.sum(got[...], axis=0), (8, LANES))
    value = value + pltpu.roll(value, KC, 1)
    value = jnp.sqrt(value / float(rows * cols * NZ * nx * ny) + norm_eps)
    norm_ref[...] = value[:1, :KC]
    pltpu.make_async_copy(others, others, norm_send).wait()


def write_kernel(residual, norms, residual_out, norms_out, sems):
    copies = [
        pltpu.make_async_copy(residual, residual_out, sems.at[0]),
        pltpu.make_async_copy(norms, norms_out, sems.at[1]),
    ]
    for c in copies:
        c.start()
    for c in copies:
        c.wait()


def body(volt, drive, region, diode_mask, sigma_table, cap_table):
    rows, cols, width = volt.shape
    regions = sigma_table.shape[0]
    nx, ny = lax.axis_size("gx"), lax.axis_size("gy")
    n = nx * ny
    region = jnp.transpose(region, (0, 2, 1))
    diode_mask = jnp.transpose(diode_mask, (0, 2, 1))
    forward, back, place = tables()
    hbm = pl.BlockSpec(memory_space=pltpu.HBM)
    vmem = pl.BlockSpec(memory_space=pltpu.VMEM)
    dma = pltpu.SemaphoreType.DMA
    residual, norms = pl.pallas_call(
        functools.partial(kernel, nx, ny, rows, cols, regions),
        out_shape=(
            pltpu.VMEM(volt.shape, jnp.float32),
            pltpu.VMEM((1, KC), jnp.float32),
        ),
        in_specs=[hbm] * 9,
        out_specs=(vmem, vmem),
        scratch_shapes=[
            pltpu.VMEM((rows + 2, cols, width), jnp.float32),
            pltpu.VMEM((rows, cols, width), jnp.float32),
            pltpu.VMEM((rows, NZ, cols), jnp.int32),
            pltpu.VMEM((rows, NZ, cols), jnp.int32),
            pltpu.VMEM((2, NZ, cols), jnp.int32),
            pltpu.VMEM((2, rows, 1, width), jnp.float32),
            pltpu.VMEM((2, rows, NZ, cols), jnp.int32),
            pltpu.SMEM((regions,), jnp.float32),
            pltpu.SMEM((regions,), jnp.float32),
            pltpu.VMEM(forward.shape, jnp.bfloat16),
            pltpu.VMEM(back.shape, jnp.bfloat16),
            pltpu.VMEM(place.shape, jnp.bfloat16),
            pltpu.VMEM((rows, NZ, LANES), jnp.float32),
            pltpu.VMEM((rows, 3, cols, LANES), jnp.bfloat16),
            pltpu.VMEM((cols, width), jnp.float32),
            pltpu.VMEM((8, width), jnp.float32),
            pltpu.VMEM((8, LANES), jnp.float32),
            pltpu.VMEM((n, 1, LANES), jnp.float32),
            dma((rows,)),
            dma((rows,)),
            dma((7,)),
            dma((2 + 2 * PIECES,)),
            dma((2 + 2 * PIECES,)),
            dma((4,)),
            dma((4,)),
            dma(()),
            dma(()),
        ],
        compiler_params=pltpu.CompilerParams(
            collective_id=0, has_side_effects=True, vmem_limit_bytes=50 * 2**20
        ),
        name="balance",
    )(volt, drive, region, diode_mask, sigma_table, cap_table, forward, back, place)
    residual, norms = pl.pallas_call(
        write_kernel,
        out_shape=(
            jax.ShapeDtypeStruct(volt.shape, jnp.float32),
            jax.ShapeDtypeStruct((1, KC), jnp.float32),
        ),
        in_specs=[vmem, vmem],
        out_specs=(hbm, hbm),
        scratch_shapes=[dma((2,))],
        compiler_params=pltpu.CompilerParams(vmem_limit_bytes=2**20),
        name="write",
    )(residual, norms)
    return residual, norms.reshape(KC)


def solution(mesh):
    return jax.shard_map(
        body,
        mesh=mesh,
        in_specs=(
            P("gx", "gy", None),
            P("gx", "gy", None),
            P("gx", "gy", None),
            P("gx", "gy", None),
            P(),
            P(),
        ),
        out_specs=(P("gx", "gy", None), P()),
        check_vma=False,
    )
```

```python
import functools
import math

import jax
import jax.numpy as jnp
import numpy as np
from jax import lax
from jax.experimental import pallas as pl
from jax.experimental.pallas import tpu as pltpu
from jax.sharding import PartitionSpec as P

NZ = 32
H = 32
KC = 64
S = 256
LANES = 128
TILES = NZ * KC // LANES
CHUNK = 16
PIECES = 1
SEND = 1

base_freq = 0.1
norm_eps = 1e-06
MESH = pl.DeviceIdType.MESH


def tables():
    orders = np.arange(1, H + 1, dtype=np.float64)
    angles = orders[:, None] * (2.0 * math.pi * np.arange(S) / S)[None, :]
    synthesis = np.concatenate([np.cos(angles), np.sin(angles)], axis=0)
    analysis = synthesis.T * (2.0 / S)
    derived = np.concatenate(
        [base_freq * orders * analysis[:, H:], -base_freq * orders * analysis[:, :H]], axis=1
    )

    def pair(table):
        zeros = np.zeros_like(table)
        return np.block([[table, zeros], [zeros, table]])

    def split(table):
        high = table.astype(jnp.bfloat16)
        low = (table - high.astype(np.float64)).astype(jnp.bfloat16)
        return high, low

    high, _ = split(pair(synthesis))
    forward = np.concatenate([high, high], axis=0)
    high, low = split(0.5 * np.concatenate([pair(analysis), pair(derived)], axis=0))
    back = np.concatenate([high, low], axis=1)
    wide = CHUNK * LANES
    place = np.zeros((4, NZ, TILES // CHUNK, 2, wide), jnp.bfloat16)
    for z in range(NZ):
        chunk, at = divmod(z * KC, wide)
        for k in range(4):
            place[k, z, chunk, k // 2, at : at + KC] = 1
    return jnp.asarray(forward), jnp.asarray(back), jnp.asarray(place.reshape(4 * NZ, -1))


def lookup(region, table, count):
    value = jnp.where(region == 0, table[0], 0.0)
    for r in range(1, count):
        value = jnp.where(region == r, table[r], value)
    return value


def harmonic_mean(left, right):
    return 2.0 * left * right / (left + right)


def packed(a, b):
    parts = []
    for g in (a, b):
        high = g.astype(jnp.bfloat16).astype(jnp.float32)
        parts += [high, g - high]
    return jnp.concatenate(parts, axis=0).T.astype(jnp.bfloat16)


def fold(value):
    return jnp.sum(value.reshape(-1, 8, LANES), axis=0)


def kernel(
    nx, ny, rows, cols, regions,
    volt_hbm, drive_hbm, region_hbm, mask_hbm, sigma_hbm, cap_hbm, forward_hbm, back_hbm, place_hbm,
    out_ref, norm_ref,
    volt_buf, drive_buf, region_buf, mask_buf, end_region, side_buf, side_region,
    sigma_ref, cap_ref, forward_ref, back_ref, place_ref, cond_buf, edge_buf, flux_buf, line_buf,
    acc_ref, got,
    volt_sem, drive_sem, misc_sem, row_send, row_recv, side_send, side_recv, norm_send, norm_recv,
):
    me_x, me_y = lax.axis_index("gx"), lax.axis_index("gy")
    up, down = lax.rem(me_x + 1, nx), lax.rem(me_x + nx - 1, nx)
    has_left, has_right = me_y > 0, me_y < ny - 1
    barrier = pltpu.get_barrier_semaphore()

    for dx in range(nx):
        for dy in range(ny):
            if dx or dy:
                peer = (lax.rem(me_x + dx, nx), lax.rem(me_y + dy, ny))
                pl.semaphore_signal(barrier, inc=1, device_id=peer, device_id_type=MESH)

    def volt_copy(row):
        return pltpu.make_async_copy(volt_hbm.at[row], volt_buf.at[row + 1], volt_sem.at[row])

    def drive_copy(row):
        return pltpu.make_async_copy(drive_hbm.at[row], drive_buf.at[row], drive_sem.at[row])

    misc = [
        pltpu.make_async_copy(region_hbm, region_buf, misc_sem.at[0]),
        pltpu.make_async_copy(mask_hbm, mask_buf, misc_sem.at[1]),
        pltpu.make_async_copy(sigma_hbm, sigma_ref, misc_sem.at[2]),
        pltpu.make_async_copy(cap_hbm, cap_ref, misc_sem.at[3]),
        pltpu.make_async_copy(forward_hbm, forward_ref, misc_sem.at[4]),
        pltpu.make_async_copy(back_hbm, back_ref, misc_sem.at[5]),
        pltpu.make_async_copy(place_hbm, place_ref, misc_sem.at[6]),
    ]
    misc[0].start()
    volt_copy(0).start()
    volt_copy(rows - 1).start()
    volt_copy(1).start()
    for c in misc[1:]:
        c.start()
    drive_copy(0).start()

    def remote(source, target, send, recv, axis, peer):
        return pltpu.make_async_remote_copy(
            src_ref=source, dst_ref=target, send_sem=send, recv_sem=recv,
            device_id={axis: peer}, device_id_type=MESH,
        )

    row_copies = [
        remote(region_buf.at[rows - 1], end_region.at[0], row_send.at[0], row_recv.at[0], "gx", up),
        remote(region_buf.at[0], end_region.at[1], row_send.at[1], row_recv.at[1], "gx", down),
    ]
    piece = TILES // PIECES * LANES
    for p in range(PIECES):
        lanes = pl.ds(p * piece, piece)
        for k, (source, target, peer) in enumerate(((rows, 0, up), (1, rows + 1, down))):
            n = 2 + 2 * p + k
            row_copies.append(remote(
                volt_buf.at[source, :, lanes], volt_buf.at[target, :, lanes],
                row_send.at[n], row_recv.at[n], "gx", peer,
            ))
    to_right = [
        remote(volt_buf.at[pl.ds(1, rows), pl.ds(cols - 1, 1), :], side_buf.at[0], side_send.at[0],
               side_recv.at[0], "gy", me_y + 1),
        remote(region_buf, side_region.at[0], side_send.at[1], side_recv.at[1], "gy", me_y + 1),
    ]
    to_left = [
        remote(volt_buf.at[pl.ds(1, rows), pl.ds(0, 1), :], side_buf.at[1], side_send.at[2],
               side_recv.at[2], "gy", me_y - 1),
        remote(region_buf, side_region.at[1], side_send.at[3], side_recv.at[3], "gy", me_y - 1),
    ]

    def send():
        for row in range(2, rows - 1):
            volt_copy(row).wait()

        @pl.when(has_right)
        def _():
            for c in to_right:
                c.start()

        @pl.when(has_left)
        def _():
            for c in to_left:
                c.start()

    volt_copy(0).wait()
    volt_copy(rows - 1).wait()
    misc[0].wait()
    pl.semaphore_wait(barrier, nx * ny - 1)
    for c in row_copies:
        c.start()
    volt_copy(1).wait()
    for c in misc[1:4]:
        c.wait()
    lane = lax.broadcasted_iota(jnp.int32, (cols, LANES), 1)
    first = lane < KC
    half = lane % KC
    order = base_freq * (half % H + 1).astype(jnp.float32)
    order = jnp.where(half < H, order, -order)
    swap = lane ^ H
    lane_t = lane[:NZ]
    depth_t = lax.broadcasted_iota(jnp.int32, (NZ, LANES), 0)

    def padded(table):
        rest = jnp.ones((NZ, LANES - cols), jnp.float32)
        return jnp.concatenate([table, rest], axis=1)

    group = LANES // cols

    def side_by_side(ref, i):
        return jnp.concatenate([ref[i + k] for k in range(group)], axis=1)

    for i in range(0, rows, group):
        cond = lookup(side_by_side(region_buf, i), sigma_ref, regions)
        cond_buf[i] = cond
        for k in range(1, group):
            cond_buf[i + k] = pltpu.roll(cond, LANES - k * cols, 1)
    for i in range(0, rows, group):
        cond = cond_buf[i]
        after = pltpu.roll(cond, LANES - cols, 1)
        later = pltpu.roll(cond_buf[min(i + group, rows - 1)], LANES - cols, 1)
        after = jnp.where(lane_t < LANES - cols, after, later)
        g_high = harmonic_mean(cond, after)
        g_col = harmonic_mean(cond, pltpu.roll(cond, LANES - 1, 1))
        g_col = jnp.where(lane_t % cols == cols - 1, 0.0, g_col)
        g_deep = harmonic_mean(cond, pltpu.roll(cond, NZ - 1, 0))
        g_deep = jnp.where(depth_t < NZ - 1, g_deep, 0.0)
        cap = lookup(side_by_side(region_buf, i), cap_ref, regions)
        diode = side_by_side(mask_buf, i).astype(jnp.float32)
        for p, edges in enumerate((packed(g_high, g_col), packed(g_deep, cap), packed(diode, diode))):
            for k in range(group):
                edge_buf[i + k, p] = edges[k * cols : (k + 1) * cols]
    for row in range(2, rows - 1):
        volt_copy(row).start()
    for row in range(1, rows):
        drive_copy(row).start()
    flux_buf[...] = jnp.zeros_like(flux_buf)
    acc_ref[...] = jnp.zeros_like(acc_ref)
    for c in misc[4:]:
        c.wait()
    wide = CHUNK * LANES

    def placed(edges, start, count=2):
        at = start * LANES * 2
        table = place_ref[:, at : at + count * wide]
        return jnp.dot(edges, table, preferred_element_type=jnp.float32)

    def row_step(i, _):
        pl.when(i == SEND)(send)
        drive_copy(i).wait()
        after = jnp.minimum(i + 2, rows)
        before = None
        total = jnp.zeros((8, LANES), jnp.float32)
        for start in range(0, TILES, CHUNK):
            xs = []
            for t in range(start, start + CHUNK):
                v = volt_buf[i + 1, :, t * LANES : (t + 1) * LANES]
                high = v.astype(jnp.bfloat16)
                low = (v - high.astype(jnp.float32)).astype(jnp.bfloat16)
                xs.append(jnp.concatenate([high, low], axis=1))
            samples = jnp.dot(
                jnp.concatenate(xs, axis=0), forward_ref[...], preferred_element_type=jnp.float32
            )
            size = jnp.maximum(samples, -samples)
            small = jnp.exp2(size * (-2.0 / math.log(2.0)) - 1.0)
            even = (size + jnp.log(0.5 + small)).astype(jnp.bfloat16)
            charge = jnp.tanh(samples.astype(jnp.bfloat16))
            projected = jnp.dot(
                jnp.concatenate([even, charge], axis=1), back_ref[...],
                preferred_element_type=jnp.float32,
            )
            projected = projected[:, :LANES] + projected[:, LANES:]
            pairs = placed(edge_buf[i, :2].reshape(2 * cols, LANES), start)
            diodes = placed(edge_buf[i, 2], start, 1)
            for t in range(start, start + CHUNK):
                at = slice(t * LANES, (t + 1) * LANES)
                one = slice((t - start) * LANES, (t - start + 1) * LANES)
                two = slice(wide + (t - start) * LANES, wide + (t - start + 1) * LANES)
                v = volt_buf[i + 1, :, at]
                flux = pairs[:cols, one] * (volt_buf[after, :, at] - v)
                value = flux_buf[:, at] - flux
                flux_buf[:, at] = flux
                flux = pairs[:cols, two] * (pltpu.roll(v, cols - 1, 0) - v)
                value += pltpu.roll(flux, 1, 0) - flux
                ahead = volt_buf[i + 1, :, (t + 1) * LANES : (t + 2) * LANES] if t + 1 < TILES else v
                deep = pltpu.roll(jnp.where(first, ahead, v), KC, 1)
                flux = pairs[cols:, one] * (deep - v)
                flux_r = pltpu.roll(flux, KC, 1)
                value += jnp.where(first, jnp.zeros_like(flux_r) if before is None else before, flux_r)
                value -= flux
                before = flux_r
                swapped = jnp.take_along_axis(v, swap, axis=1, mode="promise_in_bounds")
                value += pairs[cols:, two] * (order * swapped)
                rows_of = slice((t - start) * cols, (t - start + 1) * cols)
                value += diodes[:, one] * (projected[rows_of] + 0.5 * v)
                value -= drive_buf[i, :, at]
                out_ref[i, :, at] = value
                total += fold(value * value)
        acc_ref[...] += total
        return 0

    lax.fori_loop(0, rows, row_step, 0)

    sub8 = lax.broadcasted_iota(jnp.int32, (8, LANES), 0)

    def side(k, copies):
        for c in copies:
            c.wait_recv()
        mine, theirs = (0, cols - 1) if k == 0 else (cols - 1, 0)
        edge, line = mine // 8 * 8, mine % 8
        near = jnp.ones((NZ, LANES), jnp.float32)
        far = jnp.zeros((NZ, LANES), jnp.int32)
        for i in range(rows):
            there = jnp.concatenate([side_region[k, i]] * (LANES // cols), axis=1)
            there = pltpu.roll(there, (i - theirs) % LANES, 1)
            here = pltpu.roll(cond_buf[i], (i - mine) % LANES, 1)
            far = jnp.where(lane_t == i, there, far)
            near = jnp.where(lane_t == i, here, near)
        g = harmonic_mean(near, lookup(far, sigma_ref, regions))
        edges = packed(g, g)[:8]
        for start in range(0, TILES, CHUNK):
            line_buf[:, start * LANES : (start + CHUNK) * LANES] = placed(edges, start, 1)
        total = jnp.zeros((8, LANES), jnp.float32)
        for i in range(rows):
            for t in range(TILES):
                at = slice(t * LANES, (t + 1) * LANES)
                far = jnp.broadcast_to(side_buf[k, i, :, at], (8, LANES))
                g = jnp.broadcast_to(line_buf[i : i + 1, at], (8, LANES))
                g = jnp.where(sub8 == line, g, 0.0)
                change = g * (volt_buf[i + 1, edge : edge + 8, at] - far)
                old = out_ref[i, edge : edge + 8, at]
                out_ref[i, edge : edge + 8, at] = old + change
                total += change * (2.0 * old + change)
        acc_ref[...] += total

    pl.when(has_left)(lambda: side(0, to_right))
    pl.when(has_right)(lambda: side(1, to_left))

    row_copies[0].wait_recv()
    row_copies[1].wait_recv()
    g_low, g_high = (
        harmonic_mean(cond_buf[i], padded(lookup(end_region[k], sigma_ref, regions)))
        for k, i in ((0, 0), (1, rows - 1))
    )
    edges = packed(g_low, g_high)[:cols]
    total = acc_ref[...]
    for start in range(0, TILES, CHUNK):
        if start % (TILES // PIECES) == 0:
            for k in range(2):
                row_copies[2 + 2 * (start * PIECES // TILES) + k].wait_recv()
        ends = placed(edges, start)
        for k, i in ((0, 0), (1, rows - 1)):
            for t in range(start, start + CHUNK):
                at = slice(t * LANES, (t + 1) * LANES)
                one = slice(k * wide + (t - start) * LANES, k * wide + (t - start + 1) * LANES)
                change = ends[:, one] * (volt_buf[i + 1, :, at] - volt_buf[k * (rows + 1), :, at])
                old = out_ref[i, :, at]
                out_ref[i, :, at] = old + change
                total += fold(change * (2.0 * old + change))

    here = me_x * ny + me_y
    got[here] = jnp.sum(total, axis=0, keepdims=True)

    for c in row_copies:
        c.wait_send()

    @pl.when(has_right)
    def _():
        for c in to_right:
            c.wait_send()

    @pl.when(has_left)
    def _():
        for c in to_left:
            c.wait_send()

    peers = [(dx, dy) for dx in range(nx) for dy in range(ny) if dx or dy]
    for dx, dy in peers:
        pltpu.make_async_remote_copy(
            src_ref=got.at[here], dst_ref=got.at[here],
            send_sem=norm_send, recv_sem=norm_recv,
            device_id=(lax.rem(me_x + dx, nx), lax.rem(me_y + dy, ny)), device_id_type=MESH,
        ).start()
    others = got.at[pl.ds(0, nx * ny - 1)]
    pltpu.make_async_copy(others, others, norm_recv).wait()
    value = jnp.broadcast_to(jnp.sum(got[...], axis=0), (8, LANES))
    value = value + pltpu.roll(value, KC, 1)
    value = jnp.sqrt(value / float(rows * cols * NZ * nx * ny) + norm_eps)
    norm_ref[...] = value[:1, :KC]
    pltpu.make_async_copy(others, others, norm_send).wait()


def write_kernel(residual, norms, residual_out, norms_out, sems):
    copies = [
        pltpu.make_async_copy(residual, residual_out, sems.at[0]),
        pltpu.make_async_copy(norms, norms_out, sems.at[1]),
    ]
    for c in copies:
        c.start()
    for c in copies:
        c.wait()


def body(volt, drive, region, diode_mask, sigma_table, cap_table):
    rows, cols, width = volt.shape
    regions = sigma_table.shape[0]
    nx, ny = lax.axis_size("gx"), lax.axis_size("gy")
    n = nx * ny
    region = jnp.transpose(region, (0, 2, 1))
    diode_mask = jnp.transpose(diode_mask, (0, 2, 1))
    forward, back, place = tables()
    hbm = pl.BlockSpec(memory_space=pltpu.HBM)
    vmem = pl.BlockSpec(memory_space=pltpu.VMEM)
    dma = pltpu.SemaphoreType.DMA
    residual, norms = pl.pallas_call(
        functools.partial(kernel, nx, ny, rows, cols, regions),
        out_shape=(
            pltpu.VMEM(volt.shape, jnp.float32),
            pltpu.VMEM((1, KC), jnp.float32),
        ),
        in_specs=[hbm] * 9,
        out_specs=(vmem, vmem),
        scratch_shapes=[
            pltpu.VMEM((rows + 2, cols, width), jnp.float32),
            pltpu.VMEM((rows, cols, width), jnp.float32),
            pltpu.VMEM((rows, NZ, cols), jnp.int32),
            pltpu.VMEM((rows, NZ, cols), jnp.int32),
            pltpu.VMEM((2, NZ, cols), jnp.int32),
            pltpu.VMEM((2, rows, 1, width), jnp.float32),
            pltpu.VMEM((2, rows, NZ, cols), jnp.int32),
            pltpu.SMEM((regions,), jnp.float32),
            pltpu.SMEM((regions,), jnp.float32),
            pltpu.VMEM(forward.shape, jnp.bfloat16),
            pltpu.VMEM(back.shape, jnp.bfloat16),
            pltpu.VMEM(place.shape, jnp.bfloat16),
            pltpu.VMEM((rows, NZ, LANES), jnp.float32),
            pltpu.VMEM((rows, 3, cols, LANES), jnp.bfloat16),
            pltpu.VMEM((cols, width), jnp.float32),
            pltpu.VMEM((8, width), jnp.float32),
            pltpu.VMEM((8, LANES), jnp.float32),
            pltpu.VMEM((n, 1, LANES), jnp.float32),
            dma((rows,)),
            dma((rows,)),
            dma((7,)),
            dma((2 + 2 * PIECES,)),
            dma((2 + 2 * PIECES,)),
            dma((4,)),
            dma((4,)),
            dma(()),
            dma(()),
        ],
        compiler_params=pltpu.CompilerParams(
            collective_id=0, has_side_effects=True, vmem_limit_bytes=50 * 2**20
        ),
        name="balance",
    )(volt, drive, region, diode_mask, sigma_table, cap_table, forward, back, place)
    residual, norms = pl.pallas_call(
        write_kernel,
        out_shape=(
            jax.ShapeDtypeStruct(volt.shape, jnp.float32),
            jax.ShapeDtypeStruct((1, KC), jnp.float32),
        ),
        in_specs=[vmem, vmem],
        out_specs=(hbm, hbm),
        scratch_shapes=[dma((2,))],
        compiler_params=pltpu.CompilerParams(vmem_limit_bytes=2**20),
        name="write",
    )(residual, norms)
    return residual, norms.reshape(KC)


def solution(mesh):
    return jax.shard_map(
        body,
        mesh=mesh,
        in_specs=(
            P("gx", "gy", None),
            P("gx", "gy", None),
            P("gx", "gy", None),
            P("gx", "gy", None),
            P(),
            P(),
        ),
        out_specs=(P("gx", "gy", None), P()),
        check_vma=False,
    )
```
